32 devices in a mesh: dp: 2 (over z, core), tp: 16 (over x, y).
Axes of the slice: x: 4, y: 4, z: 1, core: 2. Of those that a mesh axis runs over, the one named last changes fastest.
The devices are a block of a 4x4x8 slice.
Arguments:
- x: bfloat16 [5120, 7168], P(('dp', 'tp')), parts along dimension 0
- w_gate: bfloat16 [7168, 20480], P(None, 'tp')
- w_up: bfloat16 [7168, 20480], P(None, 'tp')
- w_down: bfloat16 [20480, 7168], P('tp')
Outputs:
- output: bfloat16 [5120, 7168], P(('dp', 'tp')), parts along dimension 0
There are 2 independent parts. The reference program is written for one: setup_inputs(seed, part) draws one part's arguments, and reference() takes and returns one part's arrays. A program takes and returns all parts, laid end to end along the dimension named above; an argument that names none is the same for every part.
All inputs are finite; a program needn't handle non-finite values.
Results may differ from the reference program's by a relative error of at most 0.016.
Values are sent between devices in bfloat16 or wider.
A program may use at most 768 MiB of HBM per device.

```python
import jax
import jax.numpy as jnp

ROWS = 2560
D = 7168
FF = 20480


def setup_inputs(seed: int = 0, part: int = 0) -> dict:
    kx, kg, ku, kd = jax.random.split(jax.random.key(seed), 4)
    drawn = {
        "x": jax.random.normal(jax.random.fold_in(kx, part), (ROWS, D), jnp.float32),
        "w_gate": jax.random.normal(kg, (D, FF), jnp.float32) * D**-0.5,
        "w_up": jax.random.normal(ku, (D, FF), jnp.float32) * D**-0.5,
        "w_down": jax.random.normal(kd, (FF, D), jnp.float32) * FF**-0.5,
    }
    return {k: v.astype(jnp.bfloat16) for k, v in drawn.items()}


def reference(x, w_gate, w_up, w_down):
    gate = jnp.dot(x, w_gate, preferred_element_type=jnp.float32)
    up = jnp.dot(x, w_up, preferred_element_type=jnp.float32)
    hidden = (jax.nn.silu(gate) * up).astype(jnp.bfloat16)
    return jnp.dot(hidden, w_down, preferred_element_type=jnp.float32).astype(jnp.bfloat16)
```

```python
import functools
import math

import jax
import jax.numpy as jnp
from jax import lax
from jax.experimental import pallas as pl
from jax.experimental.pallas import tpu as pltpu
from jax.sharding import PartitionSpec as P

OFF = (0, 1, -1, 2)
PLUS, MINUS = 1, 2
UNITS = 8
VMEM_LIMIT = 67043328


def place(h, k, j):
    if k == 0:
        return h, j
    if k < 3:
        return 2 + j, 2 * h + k - 1
    return 6 + j // 2, 2 * h + j % 2


class Sems:
    def __init__(self):
        self.ids = {}

    def __call__(self, key):
        return self.ids.setdefault(key, len(self.ids))


def message_ids():
    ids = Sems()
    for h in (0, 1):
        for d in (0, 1):
            ids(("a", h, d)), ids(("af", h, d))
            for j in range(4):
                ids(("b", h, j, d)), ids(("bf", h, j, d))
            for k in range(4):
                for m in (1, 2, 3):
                    ids(("ra", h, k, d, m))
            for m in (1, 2, 3):
                ids(("rb", h, d, m))
    return ids.ids


IDS = message_ids()


def kernel(
    side, x, wg_hbm, wu_hbm, wd_hbm,
    y, xg, tf, tb, a1, bx, m3, rf, rb, a1b, bxb, m3b,
    wg, wu, wd, xbuf, hid, stg, fa, wsem, xsem, osem, ssem, lsem, send, recv,
):
    half, depth = x.shape[0] // 2, x.shape[1]
    piece = depth // 2
    ff = wg_hbm.shape[1]
    me = lax.axis_index("tp")
    mx, my = me // side, me % side

    def peer(h, second, d):
        step = 1 if d == 0 else side - 1
        if (h == 0) != second:
            return ((mx + step) % side) * side + my
        return mx * side + (my + step) % side

    def col(c):
        return pl.ds(c * piece, piece)

    def rows(s):
        return pl.ds(s * half, half)

    def blk(buf, h, k, j, c=None):
        u, s = place(h, k, j)
        if c is None:
            return buf.at[u, rows(s), :]
        return buf.at[u, rows(s), col(c)]

    def message(key):
        kind, h, d = key[0], key[1], key[3] if key[0] in ("b", "bf", "ra") else key[2]
        second = kind in ("b", "bf", "rb")
        here = PLUS if d == 0 else MINUS
        back = MINUS if d == 0 else PLUS
        if kind == "a":
            src, dst = x.at[rows(h), :], blk(xg, h, 0, back)
        elif kind == "af":
            src, dst = blk(xg, h, 0, back, d), blk(xg, h, 0, 3, d)
        elif kind == "b":
            j = key[2]
            src = x.at[rows(h), :] if j == 0 else blk(xg, h, 0, j)
            dst = blk(xg, h, back, j)
        elif kind == "bf":
            j = key[2]
            src, dst = blk(xg, h, back, j, d), blk(xg, h, 3, j, d)
        elif kind == "ra":
            k, m = key[2], key[4]
            if m == 1:
                src, dst = blk(tb, h, k, 3, d), a1.at[h, k, d]
            elif m == 2:
                src, dst = blk(tb, h, k, here, 1 - d), bx.at[h, k, d, :, col(1 - d)]
            else:
                src, dst = m3.at[h, k, d], bx.at[h, k, d, :, col(d)]
        else:
            m = key[3]
            if m == 1:
                src, dst = rb.at[h, 3, :, col(d)], a1b.at[h, d]
            elif m == 2:
                src, dst = rb.at[h, here, :, col(1 - d)], bxb.at[h, d, :, col(1 - d)]
            else:
                src, dst = m3b.at[h, d], bxb.at[h, d, :, col(d)]
        i = IDS[key]
        return pltpu.make_async_remote_copy(
            src_ref=src,
            dst_ref=dst,
            send_sem=send.at[i],
            recv_sem=recv.at[i],
            device_id={"tp": peer(h, second, d)},
            device_id_type=pl.DeviceIdType.MESH,
        )

    both = [(h, d) for h in (0, 1) for d in (0, 1)]

    barrier = pltpu.get_barrier_semaphore()
    for h, d in both:
        pl.semaphore_signal(
            barrier, inc=1, device_id={"tp": peer(h, False, d)},
            device_id_type=pl.DeviceIdType.MESH,
        )
    pl.semaphore_wait(barrier, 4)

    for h, d in both:
        message(("a", h, d)).start()
    weights = [
        pltpu.make_async_copy(src, dst, wsem.at[i])
        for i, (src, dst) in enumerate(((wg_hbm, wg), (wu_hbm, wu), (wd_hbm, wd)))
    ]
    own = [
        pltpu.make_async_copy(x.at[rows(h), :], xbuf.at[rows(h), :], lsem.at[h]) for h in (0, 1)
    ]
    keep = [
        pltpu.make_async_copy(xbuf.at[rows(h), :], blk(xg, h, 0, 0), lsem.at[h]) for h in (0, 1)
    ]
    for c in own:
        c.start()
    for c in own:
        c.wait()
    for c in keep:
        c.start()
    for c in weights:
        c.start()
    for c in keep:
        c.wait()
    for h, d in both:
        message(("a", h, d)).wait_recv()
        message(("af", h, d)).start()
    for j in range(3):
        for h, d in both:
            message(("b", h, j, d)).start()
    for c in weights:
        c.wait()
    for h, d in both:
        message(("af", h, d)).wait_recv()
    for h, d in both:
        message(("b", h, 3, d)).start()

    def send_terms(k):
        for m in (1, 2):
            for h, d in both:
                message(("ra", h, k, d, m)).start()

    def before(u):
        for j in range(4):
            @pl.when(u == 2 + j)
            def _():
                for h, d in both:
                    message(("b", h, j, d)).wait_recv()
                for h, d in both:
                    message(("bf", h, j, d)).start()
                if j == 3:
                    send_terms(0)

        for part in (0, 1):
            @pl.when(u == 6 + part)
            def _():
                if part == 0:
                    send_terms(PLUS)
                    send_terms(MINUS)
                for j in (2 * part, 2 * part + 1):
                    for h, d in both:
                        message(("bf", h, j, d)).wait_recv()

    n_up, n_down = 256, stg.shape[2]

    def stage(u, t, slot):
        c = pl.ds(pl.multiple_of(t * n_down, n_down), n_down)
        return pltpu.make_async_copy(stg.at[slot], tf.at[u, :, c], osem.at[slot])

    def unit(u, carry):
        before(u)
        load = pltpu.make_async_copy(xg.at[u], xbuf, xsem)
        load.start()
        load.wait()

        def up_tile(t, carry):
            c = pl.ds(pl.multiple_of(t * n_up, n_up), n_up)
            gate = jnp.dot(xbuf[...], wg[:, c], preferred_element_type=jnp.float32)
            up = jnp.dot(xbuf[...], wu[:, c], preferred_element_type=jnp.float32)
            hid[:, c] = (jax.nn.silu(gate) * up).astype(jnp.bfloat16)
            return carry

        lax.fori_loop(0, ff // n_up, up_tile, 0)
        n = depth // n_down

        def down_tile(t, carry):
            slot = t % 2

            @pl.when(t >= 2)
            def _():
                stage(u, t - 2, slot).wait()

            c = pl.ds(pl.multiple_of(t * n_down, n_down), n_down)
            term = jnp.dot(hid[...], wd[:, c], preferred_element_type=jnp.float32)
            stg[slot] = term
            xbuf[:, c] = term.astype(jnp.bfloat16)
            stage(u, t, slot).start()
            return carry

        lax.fori_loop(0, n, down_tile, 0)
        out = pltpu.make_async_copy(xbuf, tb.at[u], ssem)
        out.start()
        for t in (n - 2, n - 1):
            stage(u, t, t % 2).wait()
        out.wait()
        return carry

    lax.fori_loop(0, UNITS, unit, 0)

    def room(i):
        return xbuf.at[rows(i // 2), col(i % 2)]

    def combine(items):
        def loads(i):
            wide, narrow, _, _ = items[i]
            s = i % 2
            out = [pltpu.make_async_copy(wide, fa.at[s], lsem.at[3 * s])]
            for n, ref in enumerate(narrow):
                out.append(pltpu.make_async_copy(ref, room(3 * s + n), lsem.at[3 * s + 1 + n]))
            return out

        def stores(i):
            _, _, wide, narrow = items[i]
            s = i % 2
            out = []
            if wide is not None:
                out.append(pltpu.make_async_copy(fa.at[s], wide, osem.at[s]))
            if narrow is not None:
                out.append(pltpu.make_async_copy(room(3 * s + 2), narrow, osem.at[2 + s]))
            return out

        for c in loads(0):
            c.start()
        for i in range(len(items)):
            s = i % 2
            if i + 1 < len(items):
                if i >= 1:
                    for c in stores(i - 1):
                        c.wait()
                for c in loads(i + 1):
                    c.start()
            for c in loads(i):
                c.wait()
            total = fa[s]
            for n in range(len(items[i][1])):
                r = 3 * s + n
                total = total + xbuf[rows(r // 2), col(r % 2)].astype(jnp.float32)
            if items[i][2] is not None:
                fa[s] = total
            if items[i][3] is not None:
                r = 3 * s + 2
                xbuf[rows(r // 2), col(r % 2)] = total.astype(jnp.bfloat16)
            for c in stores(i):
                c.start()
        for i in range(max(0, len(items) - 2), len(items)):
            for c in stores(i):
                c.wait()

    def pass_on(k):
        for h, d in both:
            message(("ra", h, k, d, 1)).wait_recv()
        combine([
            (blk(tf, h, k, PLUS if d == 0 else MINUS, d), [a1.at[h, k, d]], None, m3.at[h, k, d])
            for h, d in both
        ])
        for h, d in both:
            message(("ra", h, k, d, 3)).start()

    def first_sum(k, wide, narrow):
        for h, d in both:
            for m in (2, 3):
                message(("ra", h, k, d, m)).wait_recv()
        combine([
            (
                blk(tf, h, k, 0, c),
                [bx.at[h, k, 0, :, col(c)], bx.at[h, k, 1, :, col(c)]],
                rf.at[h, k, :, col(c)] if c in wide else None,
                rb.at[h, k, :, col(c)] if c in narrow else None,
            )
            for h in (0, 1) for c in (0, 1)
        ])

    send_terms(3)
    pass_on(0)
    pass_on(PLUS)
    pass_on(3)
    pass_on(MINUS)
    first_sum(0, (0, 1), ())
    first_sum(PLUS, (0,), (1,))
    for h in (0, 1):
        message(("rb", h, 0, 2)).start()
    first_sum(3, (), (0, 1))
    for h, d in both:
        message(("rb", h, d, 1)).start()
    first_sum(MINUS, (1,), (0,))
    for h in (0, 1):
        message(("rb", h, 1, 2)).start()
    for h, d in both:
        message(("rb", h, d, 1)).wait_recv()
    combine([
        (rf.at[h, PLUS if d == 0 else MINUS, :, col(d)], [a1b.at[h, d]], None, m3b.at[h, d])
        for h, d in both
    ])
    for h, d in both:
        message(("rb", h, d, 3)).start()
    for h, d in both:
        for m in (2, 3):
            message(("rb", h, d, m)).wait_recv()
    combine([
        (
            rf.at[h, 0, :, col(c)],
            [bxb.at[h, 0, :, col(c)], bxb.at[h, 1, :, col(c)]],
            None,
            y.at[rows(h), col(c)],
        )
        for h in (0, 1) for c in (0, 1)
    ])
    for key in IDS:
        message(key).wait_send()


def solution(mesh):
    side = math.isqrt(mesh.shape["tp"])

    def step(x, w_gate, w_up, w_down):
        rows, depth = x.shape
        ff = w_gate.shape[1]
        half, piece = rows // 2, depth // 2
        bf, f32 = jnp.bfloat16, jnp.float32
        n = len(IDS)
        flops = 6 * rows * side * side * depth * ff
        shapes = [
            ((rows, depth), bf),
            ((UNITS, 4 * half, depth), bf),
            ((UNITS, 4 * half, depth), f32),
            ((UNITS, 4 * half, depth), bf),
            ((2, 4, 2, half, piece), bf),
            ((2, 4, 2, half, depth), bf),
            ((2, 4, 2, half, piece), bf),
            ((2, 4, half, depth), f32),
            ((2, 4, half, depth), bf),
            ((2, 2, half, piece), bf),
            ((2, 2, half, depth), bf),
            ((2, 2, half, piece), bf),
        ]
        out = pl.pallas_call(
            functools.partial(kernel, side),
            out_shape=[jax.ShapeDtypeStruct(s, t) for s, t in shapes],
            in_specs=[pl.BlockSpec(memory_space=pl.ANY)] * 4,
            out_specs=[pl.BlockSpec(memory_space=pl.ANY)] * len(shapes),
            scratch_shapes=[
                pltpu.VMEM((depth, ff), bf),
                pltpu.VMEM((depth, ff), bf),
                pltpu.VMEM((ff, depth), bf),
                pltpu.VMEM((4 * half, depth), bf),
                pltpu.VMEM((4 * half, ff), bf),
                pltpu.VMEM((2, 4 * half, depth // 7), f32),
                pltpu.VMEM((2, half, piece), f32),
                pltpu.SemaphoreType.DMA((3,)),
                pltpu.SemaphoreType.DMA,
                pltpu.SemaphoreType.DMA((4,)),
                pltpu.SemaphoreType.DMA,
                pltpu.SemaphoreType.DMA((6,)),
                pltpu.SemaphoreType.DMA((n,)),
                pltpu.SemaphoreType.DMA((n,)),
            ],
            compiler_params=pltpu.CompilerParams(
                collective_id=0, has_side_effects=True, vmem_limit_bytes=VMEM_LIMIT
            ),
            cost_estimate=pl.CostEstimate(
                flops=flops, bytes_accessed=3 * depth * ff * 2, transcendentals=0
            ),
            name="block",
        )(x, w_gate, w_up, w_down)
        return out[0]

    return jax.shard_map(
        step,
        mesh=mesh,
        in_specs=(P(("dp", "tp"), None), P(None, "tp"), P(None, "tp"), P("tp", None)),
        out_specs=P(("dp", "tp"), None),
        check_vma=False,
    )
```

```python
import functools
import math

import jax
import jax.numpy as jnp
from jax import lax
from jax.experimental import pallas as pl
from jax.experimental.pallas import tpu as pltpu
from jax.sharding import PartitionSpec as P

OFF = (0, 1, -1, 2)
PLUS, MINUS = 1, 2
UNITS = 8
VMEM_LIMIT = 67043328


def place(h, k, j):
    if k == 0:
        return h, j
    if k < 3:
        return 2 + j, 2 * h + k - 1
    return 6 + j // 2, 2 * h + j % 2


class Sems:
    def __init__(self):
        self.ids = {}

    def __call__(self, key):
        return self.ids.setdefault(key, len(self.ids))


def message_ids():
    ids = Sems()
    for h in (0, 1):
        for d in (0, 1):
            ids(("af", h, d))
            for c in (0, 1):
                ids(("a", h, d, c))
            for j in range(4):
                ids(("b", h, j, d)), ids(("bf", h, j, d))
            for k in range(4):
                for m in (1, 2, 3):
                    ids(("ra", h, k, d, m))
            for m in (1, 2, 3):
                ids(("rb", h, d, m))
    return ids.ids


IDS = message_ids()


def kernel(
    side, x, wg_hbm, wu_hbm, wd_hbm,
    own_sum, low, high, xg, tf, tb, a1, bx, m3, rf, rb, a1b, m3b,
    wg, wu, wd, xbuf, hid, stg, half_stg, fa, wsem, xsem, osem, ssem, lsem, send, recv,
):
    half, depth = x.shape[0] // 2, x.shape[1]
    piece = depth // 2
    ff = wg_hbm.shape[1]
    sides = (low, high)
    me = lax.axis_index("tp")
    mx, my = me // side, me % side

    def peer(h, second, d):
        step = 1 if d == 0 else side - 1
        if (h == 0) != second:
            return ((mx + step) % side) * side + my
        return mx * side + (my + step) % side

    def col(c):
        return pl.ds(c * piece, piece)

    def rows(s):
        return pl.ds(s * half, half)

    def blk(buf, h, k, j, c=None):
        u, s = place(h, k, j)
        if c is None:
            return buf.at[u, rows(s), :]
        return buf.at[u, rows(s), col(c)]

    def message(key):
        kind, h, d = key[0], key[1], key[3] if key[0] in ("b", "bf", "ra") else key[2]
        second = kind in ("b", "bf", "rb")
        here = PLUS if d == 0 else MINUS
        back = MINUS if d == 0 else PLUS
        if kind == "a":
            c = key[3]
            src, dst = x.at[rows(h), col(c)], blk(xg, h, 0, back, c)
        elif kind == "af":
            src, dst = blk(xg, h, 0, back, d), blk(xg, h, 0, 3, d)
        elif kind == "b":
            j = key[2]
            src = x.at[rows(h), :] if j == 0 else blk(xg, h, 0, j)
            dst = blk(xg, h, back, j)
        elif kind == "bf":
            j = key[2]
            src, dst = blk(xg, h, back, j, d), blk(xg, h, 3, j, d)
        elif kind == "ra":
            k, m = key[2], key[4]
            if m == 1:
                src, dst = blk(tb, h, k, 3, d), a1.at[h, k, d]
            elif m == 2:
                src, dst = blk(tb, h, k, here, 1 - d), bx.at[h, k, d, :, col(1 - d)]
            else:
                src, dst = m3.at[h, k, d], bx.at[h, k, d, :, col(d)]
        else:
            m = key[3]
            if m == 1:
                src, dst = rb.at[h, 3, :, col(d)], a1b.at[h, d]
            elif m == 2:
                src, dst = rb.at[h, here, :, col(1 - d)], sides[d].at[rows(h), col(1 - d)]
            else:
                src, dst = m3b.at[h, d], sides[d].at[rows(h), col(d)]
        i = IDS[key]
        return pltpu.make_async_remote_copy(
            src_ref=src,
            dst_ref=dst,
            send_sem=send.at[i],
            recv_sem=recv.at[i],
            device_id={"tp": peer(h, second, d)},
            device_id_type=pl.DeviceIdType.MESH,
        )

    both = [(h, d) for h in (0, 1) for d in (0, 1)]

    barrier = pltpu.get_barrier_semaphore()
    for h, d in both:
        pl.semaphore_signal(
            barrier, inc=1, device_id={"tp": peer(h, False, d)},
            device_id_type=pl.DeviceIdType.MESH,
        )
    pl.semaphore_wait(barrier, 4)

    for n in (0, 1):
        for h, d in both:
            message(("a", h, d, (d + n) % 2)).start()
    weights = [
        pltpu.make_async_copy(src, dst, wsem.at[i])
        for i, (src, dst) in enumerate(((wg_hbm, wg), (wu_hbm, wu), (wd_hbm, wd)))
    ]
    own = [
        pltpu.make_async_copy(x.at[rows(h), :], xbuf.at[rows(h), :], lsem.at[h]) for h in (0, 1)
    ]
    keep = [
        pltpu.make_async_copy(xbuf.at[rows(h), :], blk(xg, h, 0, 0), lsem.at[h]) for h in (0, 1)
    ]
    for c in own:
        c.start()
    for c in own:
        c.wait()
    for c in keep:
        c.start()
    for c in weights:
        c.start()
    for c in keep:
        c.wait()
    for h, d in both:
        message(("a", h, d, d)).wait_recv()
        message(("af", h, d)).start()
    for h, d in both:
        message(("b", h, 0, d)).start()
    for h, d in both:
        message(("a", h, d, 1 - d)).wait_recv()
    for j in (PLUS, MINUS):
        for h, d in both:
            message(("b", h, j, d)).start()
    for c in weights:
        c.wait()
    for h, d in both:
        message(("af", h, d)).wait_recv()
    for h, d in both:
        message(("b", h, 3, d)).start()

    def send_terms(k):
        for m in (1, 2):
            for h, d in both:
                message(("ra", h, k, d, m)).start()

    def arrivals(u):
        for j in range(4):
            @pl.when(u == 1 + j)
            def _():
                for h, d in both:
                    message(("b", h, j, d)).wait_recv()
                    message(("bf", h, j, d)).start()
                if j == 3:
                    send_terms(0)

        for part in (0, 1):
            @pl.when(u == 5 + part)
            def _():
                if part == 1:
                    send_terms(PLUS)
                    send_terms(MINUS)
                for j in (2 * part, 2 * part + 1):
                    for h, d in both:
                        message(("bf", h, j, d)).wait_recv()

    n_up, n_down = 256, stg.shape[2]
    n = depth // n_down

    def stage(u, t, slot):
        c = pl.ds(pl.multiple_of(t * n_down, n_down), n_down)
        return (
            pltpu.make_async_copy(stg.at[slot], tf.at[u, :, c], osem.at[slot]),
            pltpu.make_async_copy(half_stg.at[slot], tb.at[u, :, c], ssem.at[slot]),
        )

    def drain(u):
        for t in (n - 2, n - 1):
            for c in stage(u, t, t % 2):
                c.wait()

    def load(u):
        return pltpu.make_async_copy(xg.at[u], xbuf, xsem)

    load(0).start()

    def unit(u, carry):
        load(u).wait()

        def up_tile(t, carry):
            c = pl.ds(pl.multiple_of(t * n_up, n_up), n_up)
            gate = jnp.dot(xbuf[...], wg[:, c], preferred_element_type=jnp.float32)
            up = jnp.dot(xbuf[...], wu[:, c], preferred_element_type=jnp.float32)
            hid[:, c] = (jax.nn.silu(gate) * up).astype(jnp.bfloat16)
            return carry

        lax.fori_loop(0, ff // n_up, up_tile, 0)

        @pl.when(u > 0)
        def _():
            drain(u - 1)

        arrivals(u)

        @pl.when(u < UNITS - 1)
        def _():
            load(u + 1).start()

        def down_tile(t, carry):
            slot = t % 2

            @pl.when(t >= 2)
            def _():
                for c in stage(u, t - 2, slot):
                    c.wait()

            c = pl.ds(pl.multiple_of(t * n_down, n_down), n_down)
            term = jnp.dot(hid[...], wd[:, c], preferred_element_type=jnp.float32)
            stg[slot] = term
            half_stg[slot] = term.astype(jnp.bfloat16)
            for c in stage(u, t, slot):
                c.start()
            return carry

        lax.fori_loop(0, n, down_tile, 0)
        return carry

    lax.fori_loop(0, UNITS, unit, 0)
    drain(UNITS - 1)

    quarter = fa.shape[2]

    def room(i):
        return rows(i // 4), pl.ds((i % 4) * quarter, quarter)

    def combine(items):
        parts = []
        for wide, narrow, to_wide, to_narrow, then in items:
            for q in (0, 1):
                c = pl.ds(q * quarter, quarter)
                cut = lambda ref: None if ref is None else ref.at[:, c]
                parts.append((
                    cut(wide), [cut(r) for r in narrow], cut(to_wide), cut(to_narrow),
                    then if q == 1 else None,
                ))

        def loads(i):
            wide, narrow = parts[i][:2]
            s = i % 2
            out = [pltpu.make_async_copy(wide, fa.at[s], lsem.at[3 * s])]
            for n, ref in enumerate(narrow):
                out.append(pltpu.make_async_copy(
                    ref, xbuf.at[room(3 * s + n)], lsem.at[3 * s + 1 + n]))
            return out

        def stores(i):
            wide, narrow = parts[i][2:4]
            s = i % 2
            out = []
            if wide is not None:
                out.append(pltpu.make_async_copy(fa.at[s], wide, osem.at[s]))
            if narrow is not None:
                out.append(pltpu.make_async_copy(xbuf.at[room(3 * s + 2)], narrow, ssem.at[s]))
            return out

        def finish(i):
            for c in stores(i):
                c.wait()
            if parts[i][4] is not None:
                parts[i][4].start()

        for c in loads(0):
            c.start()
        for i in range(len(parts)):
            s = i % 2
            if i >= 1:
                finish(i - 1)
            if i + 1 < len(parts):
                for c in loads(i + 1):
                    c.start()
            for c in loads(i):
                c.wait()
            total = fa[s]
            for n in range(len(parts[i][1])):
                total = total + xbuf[room(3 * s + n)].astype(jnp.float32)
            if parts[i][2] is not None:
                fa[s] = total
            if parts[i][3] is not None:
                xbuf[room(3 * s + 2)] = total.astype(jnp.bfloat16)
            for c in stores(i):
                c.start()
        finish(len(parts) - 1)

    def pass_on(k):
        for h, d in both:
            message(("ra", h, k, d, 1)).wait_recv()
        combine([
            (
                blk(tf, h, k, PLUS if d == 0 else MINUS, d), [a1.at[h, k, d]],
                None, m3.at[h, k, d], message(("ra", h, k, d, 3)),
            )
            for h, d in both
        ])

    def first_sum(k, wide, narrow, then=lambda h, c: None):
        for h, d in both:
            for m in (2, 3):
                message(("ra", h, k, d, m)).wait_recv()
        combine([
            (
                blk(tf, h, k, 0, c),
                [bx.at[h, k, 0, :, col(c)], bx.at[h, k, 1, :, col(c)]],
                (own_sum.at[rows(h), col(c)] if k == 0 else rf.at[h, k, :, col(c)])
                if c in wide else None,
                rb.at[h, k, :, col(c)] if c in narrow else None,
                then(h, c),
            )
            for h in (0, 1) for c in (0, 1)
        ])

    send_terms(3)
    pass_on(0)
    pass_on(PLUS)
    pass_on(3)
    pass_on(MINUS)
    first_sum(0, (0, 1), ())
    first_sum(PLUS, (0,), (1,))
    first_sum(3, (), (0, 1), lambda h, c: message(("rb", h, c, 1)))
    for h in (0, 1):
        message(("rb", h, 0, 2)).start()
    first_sum(MINUS, (1,), (0,), lambda h, c: message(("rb", h, 1, 2)) if c == 0 else None)
    for h, d in both:
        message(("rb", h, d, 1)).wait_recv()
    combine([
        (
            rf.at[h, PLUS if d == 0 else MINUS, :, col(d)], [a1b.at[h, d]],
            None, m3b.at[h, d], message(("rb", h, d, 3)),
        )
        for h, d in both
    ])
    for h, d in both:
        for m in (2, 3):
            message(("rb", h, d, m)).wait_recv()
    for key in IDS:
        message(key).wait_send()


def solution(mesh):
    side = math.isqrt(mesh.shape["tp"])

    def step(x, w_gate, w_up, w_down):
        rows, depth = x.shape
        ff = w_gate.shape[1]
        half, piece = rows // 2, depth // 2
        bf, f32 = jnp.bfloat16, jnp.float32
        n = len(IDS)
        flops = 6 * rows * side * side * depth * ff
        shapes = [
            ((rows, depth), f32),
            ((rows, depth), bf),
            ((rows, depth), bf),
            ((UNITS, 4 * half, depth), bf),
            ((UNITS, 4 * half, depth), f32),
            ((UNITS, 4 * half, depth), bf),
            ((2, 4, 2, half, piece), bf),
            ((2, 4, 2, half, depth), bf),
            ((2, 4, 2, half, piece), bf),
            ((2, 4, half, depth), f32),
            ((2, 4, half, depth), bf),
            ((2, 2, half, piece), bf),
            ((2, 2, half, piece), bf),
        ]
        out = pl.pallas_call(
            functools.partial(kernel, side),
            out_shape=[jax.ShapeDtypeStruct(s, t) for s, t in shapes],
            in_specs=[pl.BlockSpec(memory_space=pl.ANY)] * 4,
            out_specs=[pl.BlockSpec(memory_space=pl.ANY)] * len(shapes),
            scratch_shapes=[
                pltpu.VMEM((depth, ff), bf),
                pltpu.VMEM((depth, ff), bf),
                pltpu.VMEM((ff, depth), bf),
                pltpu.VMEM((4 * half, depth), bf),
                pltpu.VMEM((4 * half, ff), bf),
                pltpu.VMEM((2, 4 * half, depth // 7), f32),
                pltpu.VMEM((2, 4 * half, depth // 7), bf),
                pltpu.VMEM((2, half, piece // 2), f32),
                pltpu.SemaphoreType.DMA((3,)),
                pltpu.SemaphoreType.DMA,
                pltpu.SemaphoreType.DMA((2,)),
                pltpu.SemaphoreType.DMA((2,)),
                pltpu.SemaphoreType.DMA((6,)),
                pltpu.SemaphoreType.DMA((n,)),
                pltpu.SemaphoreType.DMA((n,)),
            ],
            compiler_params=pltpu.CompilerParams(
                collective_id=0, has_side_effects=True, vmem_limit_bytes=VMEM_LIMIT
            ),
            cost_estimate=pl.CostEstimate(
                flops=flops, bytes_accessed=3 * depth * ff * 2, transcendentals=0
            ),
            name="block",
        )(x, w_gate, w_up, w_down)
        own_sum, low, high = out[:3]
        return (own_sum + low.astype(f32) + high.astype(f32)).astype(bf)

    return jax.shard_map(
        step,
        mesh=mesh,
        in_specs=(P(("dp", "tp"), None), P(None, "tp"), P(None, "tp"), P("tp", None)),
        out_specs=P(("dp", "tp"), None),
        check_vma=False,
    )
```

```python
import functools
import math

import jax
import jax.numpy as jnp
from jax import lax
from jax.experimental import pallas as pl
from jax.experimental.pallas import tpu as pltpu
from jax.sharding import PartitionSpec as P

OFF = (0, 1, -1, 2)
PLUS, MINUS = 1, 2
LATE = 1536
UNITS = 8
VMEM_LIMIT = 67043328


def place(h, k, j):
    if k == 0:
        return h, j
    if k < 3:
        return 2 + j, 2 * h + k - 1
    return 6 + j // 2, 2 * h + j % 2


class Sems:
    def __init__(self):
        self.ids = {}

    def __call__(self, key):
        return self.ids.setdefault(key, len(self.ids))


def message_ids():
    ids = Sems()
    for h in (0, 1):
        for d in (0, 1):
            ids(("af", h, d))
            for c in (0, 1):
                ids(("a", h, d, c))
            for j in range(4):
                ids(("b", h, j, d)), ids(("bf", h, j, d))
            for k in range(4):
                for m in (1, 2, 3):
                    ids(("ra", h, k, d, m))
            for m in (1, 2, 3, 4):
                ids(("rb", h, d, m))
    return ids.ids


IDS = message_ids()


def kernel(
    side, x, wg_hbm, wu_hbm, wd_hbm,
    early, most, late, xg, tf, tb, a1, bx, m3, rf, rb, a1b, m3b, mid, near,
    wg, wu, wd, xbuf, hid, stg, half_stg, fa, wsem, xsem, osem, ssem, lsem, zsem, send, recv,
):
    half, depth = x.shape[0] // 2, x.shape[1]
    piece = depth // 2
    soon = piece - LATE
    ff = wg_hbm.shape[1]
    me = lax.axis_index("tp")
    mx, my = me // side, me % side

    def peer(h, second, d):
        step = 1 if d == 0 else side - 1
        if (h == 0) != second:
            return ((mx + step) % side) * side + my
        return mx * side + (my + step) % side

    def col(c):
        return pl.ds(c * piece, piece)

    def rows(s):
        return pl.ds(s * half, half)

    def blk(buf, h, k, j, c=None):
        u, s = place(h, k, j)
        if c is None:
            return buf.at[u, rows(s), :]
        return buf.at[u, rows(s), col(c)]

    def message(key):
        kind, h, d = key[0], key[1], key[3] if key[0] in ("b", "bf", "ra") else key[2]
        second = kind in ("b", "bf", "rb")
        here = PLUS if d == 0 else MINUS
        back = MINUS if d == 0 else PLUS
        if kind == "a":
            c = key[3]
            src, dst = x.at[rows(h), col(c)], blk(xg, h, 0, back, c)
        elif kind == "af":
            src, dst = blk(xg, h, 0, back, d), blk(xg, h, 0, 3, d)
        elif kind == "b":
            j = key[2]
            src = x.at[rows(h), :] if j == 0 else blk(xg, h, 0, j)
            dst = blk(xg, h, back, j)
        elif kind == "bf":
            j = key[2]
            src, dst = blk(xg, h, back, j, d), blk(xg, h, 3, j, d)
        elif kind == "ra":
            k, m = key[2], key[4]
            if m == 1:
                src, dst = blk(tb, h, k, 3, d), a1.at[h, k, d]
            elif m == 2:
                src, dst = blk(tb, h, k, here, 1 - d), bx.at[h, k, d, :, col(1 - d)]
            else:
                src, dst = m3.at[h, k, d], bx.at[h, k, d, :, col(d)]
        else:
            m = key[3]
            if m == 1:
                src, dst = rb.at[h, 3, :, col(d)], a1b.at[h, d]
            elif m == 2:
                src, dst = rb.at[h, here, :, col(1 - d)], mid.at[h, d]
            elif m == 3:
                src, dst = m3b.at[h, d, :, pl.ds(0, soon)], near.at[h, d]
            else:
                src = m3b.at[h, d, :, pl.ds(soon, LATE)]
                dst = late.at[rows(h), pl.ds(d * LATE, LATE)]
        i = IDS[key]
        return pltpu.make_async_remote_copy(
            src_ref=src,
            dst_ref=dst,
            send_sem=send.at[i],
            recv_sem=recv.at[i],
            device_id={"tp": peer(h, second, d)},
            device_id_type=pl.DeviceIdType.MESH,
        )

    both = [(h, d) for h in (0, 1) for d in (0, 1)]

    barrier = pltpu.get_barrier_semaphore()
    for h, d in both:
        pl.semaphore_signal(
            barrier, inc=1, device_id={"tp": peer(h, False, d)},
            device_id_type=pl.DeviceIdType.MESH,
        )
    pl.semaphore_wait(barrier, 4)

    for n in (0, 1):
        for h, d in both:
            message(("a", h, d, (d + n) % 2)).start()
    weights = [
        pltpu.make_async_copy(src, dst, wsem.at[i])
        for i, (src, dst) in enumerate(((wg_hbm, wg), (wu_hbm, wu), (wd_hbm, wd)))
    ]
    own = [
        pltpu.make_async_copy(x.at[rows(h), :], xbuf.at[rows(h), :], lsem.at[h]) for h in (0, 1)
    ]
    keep = [
        pltpu.make_async_copy(xbuf.at[rows(h), :], blk(xg, h, 0, 0), lsem.at[h]) for h in (0, 1)
    ]
    for c in own:
        c.start()
    for c in own:
        c.wait()
    for c in keep:
        c.start()
    for c in weights:
        c.start()
    for c in keep:
        c.wait()
    for h, d in both:
        message(("a", h, d, d)).wait_recv()
        message(("af", h, d)).start()
    for h, d in both:
        message(("b", h, 0, d)).start()
    for h, d in both:
        message(("a", h, d, 1 - d)).wait_recv()
    for j in (PLUS, MINUS):
        for h, d in both:
            message(("b", h, j, d)).start()
    for c in weights:
        c.wait()
    for h, d in both:
        message(("af", h, d)).wait_recv()
    for h, d in both:
        message(("b", h, 3, d)).start()

    def send_terms(k):
        for m in (1, 2):
            for h, d in both:
                message(("ra", h, k, d, m)).start()

    def arrivals(u):
        for j in range(4):
            @pl.when(u == 1 + j)
            def _():
                for h, d in both:
                    message(("b", h, j, d)).wait_recv()
                    message(("bf", h, j, d)).start()
                if j == 3:
                    send_terms(0)

        for part in (0, 1):
            @pl.when(u == 5 + part)
            def _():
                if part == 1:
                    send_terms(PLUS)
                    send_terms(MINUS)
                for j in (2 * part, 2 * part + 1):
                    for h, d in both:
                        message(("bf", h, j, d)).wait_recv()

    n_up, n_down = 256, stg.shape[2]
    n = depth // n_down

    def stage(u, t, slot):
        c = pl.ds(pl.multiple_of(t * n_down, n_down), n_down)
        return (
            pltpu.make_async_copy(stg.at[slot], tf.at[u, :, c], osem.at[slot]),
            pltpu.make_async_copy(half_stg.at[slot], tb.at[u, :, c], ssem.at[slot]),
        )

    def drain(u):
        for t in (n - 2, n - 1):
            for c in stage(u, t, t % 2):
                c.wait()

    def load(u):
        return pltpu.make_async_copy(xg.at[u], xbuf, xsem)

    load(0).start()

    def unit(u, carry):
        load(u).wait()

        def up_tile(t, carry):
            c = pl.ds(pl.multiple_of(t * n_up, n_up), n_up)
            gate = jnp.dot(xbuf[...], wg[:, c], preferred_element_type=jnp.float32)
            up = jnp.dot(xbuf[...], wu[:, c], preferred_element_type=jnp.float32)
            hid[:, c] = (jax.nn.silu(gate) * up).astype(jnp.bfloat16)
            return carry

        lax.fori_loop(0, ff // n_up, up_tile, 0)

        @pl.when(u > 0)
        def _():
            drain(u - 1)

        arrivals(u)

        @pl.when(u < UNITS - 1)
        def _():
            load(u + 1).start()

        def down_tile(t, carry):
            slot = t % 2

            @pl.when(t >= 2)
            def _():
                for c in stage(u, t - 2, slot):
                    c.wait()

            c = pl.ds(pl.multiple_of(t * n_down, n_down), n_down)
            term = jnp.dot(hid[...], wd[:, c], preferred_element_type=jnp.float32)
            stg[slot] = term
            half_stg[slot] = term.astype(jnp.bfloat16)
            for c in stage(u, t, slot):
                c.start()
            return carry

        lax.fori_loop(0, n, down_tile, 0)
        return carry

    lax.fori_loop(0, UNITS, unit, 0)
    drain(UNITS - 1)

    quarter = fa.shape[2]

    def combine(items, wide_columns=piece):
        step = min(quarter, wide_columns)

        def room(i):
            return rows(i // 4), pl.ds((i % 4) * quarter, step)

        parts = []
        for wide, narrow, to_wide, to_narrow, then in items:
            for q in range(wide_columns // step):
                c = pl.ds(q * step, step)
                cut = lambda ref: None if ref is None else ref.at[:, c]
                parts.append((
                    cut(wide), [cut(r) for r in narrow], cut(to_wide), cut(to_narrow),
                    then if q == wide_columns // step - 1 else None,
                ))

        def loads(i):
            wide, narrow = parts[i][:2]
            s = i % 2
            out = [pltpu.make_async_copy(wide, fa.at[s, :, pl.ds(0, step)], lsem.at[3 * s])]
            for n, ref in enumerate(narrow):
                out.append(pltpu.make_async_copy(
                    ref, xbuf.at[room(3 * s + n)], lsem.at[3 * s + 1 + n]))
            return out

        def stores(i):
            wide, narrow = parts[i][2:4]
            s = i % 2
            out = []
            if wide is not None:
                out.append(pltpu.make_async_copy(fa.at[s, :, pl.ds(0, step)], wide, osem.at[s]))
            if narrow is not None:
                out.append(pltpu.make_async_copy(xbuf.at[room(3 * s + 2)], narrow, ssem.at[s]))
            return out

        def finish(i):
            for c in stores(i):
                c.wait()
            if parts[i][4] is not None:
                parts[i][4].start()

        for c in loads(0):
            c.start()
        for i in range(len(parts)):
            s = i % 2
            if i >= 1:
                finish(i - 1)
            if i + 1 < len(parts):
                for c in loads(i + 1):
                    c.start()
            for c in loads(i):
                c.wait()
            total = fa[s, :, :step]
            for n in range(len(parts[i][1])):
                total = total + xbuf[room(3 * s + n)].astype(jnp.float32)
            if parts[i][2] is not None:
                fa[s, :, :step] = total
            if parts[i][3] is not None:
                xbuf[room(3 * s + 2)] = total.astype(jnp.bfloat16)
            for c in stores(i):
                c.start()
        finish(len(parts) - 1)

    def pass_on(k):
        for h, d in both:
            message(("ra", h, k, d, 1)).wait_recv()
        combine([
            (
                blk(tf, h, k, PLUS if d == 0 else MINUS, d), [a1.at[h, k, d]],
                None, m3.at[h, k, d], message(("ra", h, k, d, 3)),
            )
            for h, d in both
        ])

    def first_sum(k, wide, narrow, then=lambda h, c: None):
        for h, d in both:
            for m in (2, 3):
                message(("ra", h, k, d, m)).wait_recv()
        combine([
            (
                blk(tf, h, k, 0, c),
                [bx.at[h, k, 0, :, col(c)], bx.at[h, k, 1, :, col(c)]],
                rf.at[h, k, :, col(c)] if c in wide else None,
                rb.at[h, k, :, col(c)] if c in narrow else None,
                then(h, c),
            )
            for h in (0, 1) for c in (0, 1)
        ])

    send_terms(3)
    pass_on(0)
    pass_on(PLUS)
    pass_on(3)
    pass_on(MINUS)
    first_sum(0, (0, 1), ())
    first_sum(PLUS, (0,), (1,))
    first_sum(3, (), (0, 1), lambda h, c: message(("rb", h, c, 1)))
    for h in (0, 1):
        message(("rb", h, 0, 2)).start()
    first_sum(MINUS, (1,), (0,), lambda h, c: message(("rb", h, 1, 2)) if c == 0 else None)
    for h, d in both:
        message(("rb", h, d, 1)).wait_recv()
    combine([
        (
            rf.at[h, PLUS if d == 0 else MINUS, :, col(d)], [a1b.at[h, d]],
            None, m3b.at[h, d], message(("rb", h, d, 3)),
        )
        for h, d in both
    ])
    for h, d in both:
        message(("rb", h, d, 4)).start()

    for h, d in both:
        message(("rb", h, d, 2)).wait_recv()
    width = n_down
    spots = [(h, c, q) for h in (0, 1) for c in (0, 1) for q in range(soon // width)]

    def spot(i):
        h, c, q = spots[i]
        return q, rows(2 * h + c)

    def lane(i):
        h, c, q = spots[i]
        return rows(2 * h + c), pl.ds(q * width, width)

    def fetch(i):
        h, c, q = spots[i]
        return (
            pltpu.make_async_copy(
                rf.at[h, 0, :, pl.ds(c * piece + q * width, width)], stg.at[spot(i)], zsem.at[i]),
            pltpu.make_async_copy(
                mid.at[h, 1 - c, :, pl.ds(q * width, width)], xbuf.at[lane(i)],
                zsem.at[len(spots) + i]),
        )

    for i in range(len(spots)):
        for c in fetch(i):
            c.start()
    for i in range(len(spots)):
        for c in fetch(i):
            c.wait()
        stg[spot(i)] = stg[spot(i)] + xbuf[lane(i)].astype(jnp.float32)
    combine([
        (
            rf.at[h, 0, :, pl.ds(c * piece + soon, LATE)],
            [mid.at[h, 1 - c, :, pl.ds(soon, LATE)]],
            most.at[rows(h), pl.ds(c * LATE, LATE)], None, None,
        )
        for h in (0, 1) for c in (0, 1)
    ], LATE)
    for h, d in both:
        message(("rb", h, d, 3)).wait_recv()

    def arrived(i):
        h, c, q = spots[i]
        return pltpu.make_async_copy(
            near.at[h, c, :, pl.ds(q * width, width)], xbuf.at[lane(i)], zsem.at[i])

    def settled(i):
        h, c, q = spots[i]
        return pltpu.make_async_copy(
            xbuf.at[lane(i)], early.at[rows(h), pl.ds(c * soon + q * width, width)],
            zsem.at[len(spots) + i])

    for i in range(len(spots)):
        arrived(i).start()
    for i in range(len(spots)):
        arrived(i).wait()
        total = stg[spot(i)] + xbuf[lane(i)].astype(jnp.float32)
        xbuf[lane(i)] = total.astype(jnp.bfloat16)
        settled(i).start()
    for i in range(len(spots)):
        settled(i).wait()
    for h, d in both:
        message(("rb", h, d, 4)).wait_recv()
    for key in IDS:
        message(key).wait_send()


def finish(early, most, late, y, rest, add, out, sem):
    rows, columns = most.shape
    piece, soon, cut = y.shape[1] // 2, early.shape[1] // 2, rows // 2
    spots = [(i, c) for i in (0, 1) for c in (0, 1)]

    def part(i, c, n):
        r = pl.ds(i * cut, cut)
        place = (r, pl.ds(c * piece, soon))
        lane = (r, pl.ds(c * LATE, LATE))
        to = (r, pl.ds(c * piece + soon, LATE))
        src, dst = (
            (most.at[lane], rest.at[lane]),
            (late.at[lane], add.at[lane]),
            (early.at[r, pl.ds(c * soon, soon)], out.at[place]),
            (out.at[place], y.at[place]),
            (out.at[to], y.at[to]),
        )[n]
        return pltpu.make_async_copy(src, dst, sem.at[5 * (2 * i + c) + n])

    for i, c in spots:
        for n in (0, 1, 2):
            part(i, c, n).start()
    for i, c in spots:
        part(i, c, 0).wait()
        part(i, c, 1).wait()
        r, lane = pl.ds(i * cut, cut), pl.ds(c * LATE, LATE)
        total = rest[r, lane] + add[r, lane].astype(jnp.float32)
        out[r, pl.ds(c * piece + soon, LATE)] = total.astype(out.dtype)
        part(i, c, 4).start()
        part(i, c, 2).wait()
        part(i, c, 3).start()
    for i, c in spots:
        part(i, c, 3).wait()
        part(i, c, 4).wait()


def solution(mesh):
    side = math.isqrt(mesh.shape["tp"])

    def step(x, w_gate, w_up, w_down):
        rows, depth = x.shape
        ff = w_gate.shape[1]
        half, piece = rows // 2, depth // 2
        bf, f32 = jnp.bfloat16, jnp.float32
        n = len(IDS)
        flops = 6 * rows * side * side * depth * ff
        shapes = [
            ((rows, depth - 2 * LATE), bf),
            ((rows, 2 * LATE), f32),
            ((rows, 2 * LATE), bf),
            ((UNITS, 4 * half, depth), bf),
            ((UNITS, 4 * half, depth), f32),
            ((UNITS, 4 * half, depth), bf),
            ((2, 4, 2, half, piece), bf),
            ((2, 4, 2, half, depth), bf),
            ((2, 4, 2, half, piece), bf),
            ((2, 4, half, depth), f32),
            ((2, 4, half, depth), bf),
            ((2, 2, half, piece), bf),
            ((2, 2, half, piece), bf),
            ((2, 2, half, piece), bf),
            ((2, 2, half, piece - LATE), bf),
        ]
        out = pl.pallas_call(
            functools.partial(kernel, side),
            out_shape=[jax.ShapeDtypeStruct(s, t) for s, t in shapes],
            in_specs=[pl.BlockSpec(memory_space=pl.ANY)] * 4,
            out_specs=[pl.BlockSpec(memory_space=pl.ANY)] * len(shapes),
            scratch_shapes=[
                pltpu.VMEM((depth, ff), bf),
                pltpu.VMEM((depth, ff), bf),
                pltpu.VMEM((ff, depth), bf),
                pltpu.VMEM((4 * half, depth), bf),
                pltpu.VMEM((4 * half, ff), bf),
                pltpu.VMEM((2, 4 * half, depth // 7), f32),
                pltpu.VMEM((2, 4 * half, depth // 7), bf),
                pltpu.VMEM((2, half, piece // 2), f32),
                pltpu.SemaphoreType.DMA((3,)),
                pltpu.SemaphoreType.DMA,
                pltpu.SemaphoreType.DMA((2,)),
                pltpu.SemaphoreType.DMA((2,)),
                pltpu.SemaphoreType.DMA((6,)),
                pltpu.SemaphoreType.DMA((16,)),
                pltpu.SemaphoreType.DMA((n,)),
                pltpu.SemaphoreType.DMA((n,)),
            ],
            compiler_params=pltpu.CompilerParams(
                collective_id=0, has_side_effects=True, vmem_limit_bytes=VMEM_LIMIT
            ),
            cost_estimate=pl.CostEstimate(
                flops=flops, bytes_accessed=3 * depth * ff * 2, transcendentals=0
            ),
            name="block",
        )(x, w_gate, w_up, w_down)
        return pl.pallas_call(
            finish,
            out_shape=jax.ShapeDtypeStruct((rows, depth), bf),
            in_specs=[pl.BlockSpec(memory_space=pl.ANY)] * 3,
            out_specs=pl.BlockSpec(memory_space=pl.ANY),
            scratch_shapes=[
                pltpu.VMEM((rows, 2 * LATE), f32),
                pltpu.VMEM((rows, 2 * LATE), bf),
                pltpu.VMEM((rows, depth), bf),
                pltpu.SemaphoreType.DMA((20,)),
            ],
            compiler_params=pltpu.CompilerParams(vmem_limit_bytes=VMEM_LIMIT),
            name="finish",
        )(*out[:3])

    return jax.shard_map(
        step,
        mesh=mesh,
        in_specs=(P(("dp", "tp"), None), P(None, "tp"), P(None, "tp"), P("tp", None)),
        out_specs=P(("dp", "tp"), None),
        check_vma=False,
    )
```

```python
import functools
import math

import jax
import jax.numpy as jnp
from jax import lax
from jax.experimental import pallas as pl
from jax.experimental.pallas import tpu as pltpu
from jax.sharding import PartitionSpec as P

OFF = (0, 1, -1, 2)
PLUS, MINUS = 1, 2
LATE = 1536
UNITS = 8
VMEM_LIMIT = 67043328


def place(h, k, j):
    if k == 0:
        return h, j
    if k < 3:
        return 2 + j, 2 * h + k - 1
    return 6 + j // 2, 2 * h + j % 2


class Sems:
    def __init__(self):
        self.ids = {}

    def __call__(self, key):
        return self.ids.setdefault(key, len(self.ids))


def message_ids():
    ids = Sems()
    for h in (0, 1):
        for d in (0, 1):
            ids(("af", h, d))
            for c in (0, 1):
                ids(("a", h, d, c))
            for j in range(4):
                ids(("b", h, j, d)), ids(("bf", h, j, d))
            for k in range(4):
                for m in (1, 2, 3):
                    ids(("ra", h, k, d, m))
            for m in (1, 2, 3, 4):
                ids(("rb", h, d, m))
    return ids.ids


IDS = message_ids()


def kernel(
    side, x, wg_hbm, wu_hbm, wd_hbm,
    early, most, late, xg, tf, tb, a1, bx, m3, rf, rb, a1b, m3b, mid, near,
    wg, wu, wd, xbuf, hid, stg, half_stg, fa, wsem, xsem, osem, ssem, lsem, zsem, below, send, recv,
):
    half, depth = x.shape[0] // 2, x.shape[1]
    piece = depth // 2
    soon = piece - LATE
    ff = wg_hbm.shape[1]
    me = lax.axis_index("tp")
    mx, my = me // side, me % side

    def peer(h, second, d):
        step = 1 if d == 0 else side - 1
        if (h == 0) != second:
            return ((mx + step) % side) * side + my
        return mx * side + (my + step) % side

    def col(c):
        return pl.ds(c * piece, piece)

    def rows(s):
        return pl.ds(s * half, half)

    def blk(buf, h, k, j, c=None):
        u, s = place(h, k, j)
        if c is None:
            return buf.at[u, rows(s), :]
        return buf.at[u, rows(s), col(c)]

    def message(key):
        kind, h, d = key[0], key[1], key[3] if key[0] in ("b", "bf", "ra") else key[2]
        second = kind in ("b", "bf", "rb")
        here = PLUS if d == 0 else MINUS
        back = MINUS if d == 0 else PLUS
        if kind == "a":
            c = key[3]
            src, dst = x.at[rows(h), col(c)], blk(xg, h, 0, back, c)
        elif kind == "af":
            src, dst = blk(xg, h, 0, back, d), blk(xg, h, 0, 3, d)
        elif kind == "b":
            j = key[2]
            src = x.at[rows(h), :] if j == 0 else blk(xg, h, 0, j)
            dst = blk(xg, h, back, j)
        elif kind == "bf":
            j = key[2]
            src, dst = blk(xg, h, back, j, d), blk(xg, h, 3, j, d)
        elif kind == "ra":
            k, m = key[2], key[4]
            if m == 1:
                src, dst = blk(tb, h, k, 3, d), a1.at[h, k, d]
            elif m == 2:
                src, dst = blk(tb, h, k, here, 1 - d), bx.at[h, k, d, :, col(1 - d)]
            else:
                src, dst = m3.at[h, k, d], bx.at[h, k, d, :, col(d)]
        else:
            m = key[3]
            if m == 1:
                src, dst = rb.at[h, 3, :, col(d)], a1b.at[h, d]
            elif m == 2:
                src, dst = rb.at[h, here, :, col(1 - d)], mid.at[h, d]
            elif m == 3:
                src, dst = m3b.at[h, d, :, pl.ds(0, soon)], near.at[h, d]
            else:
                src = m3b.at[h, d, :, pl.ds(soon, LATE)]
                dst = late.at[rows(h), pl.ds(d * LATE, LATE)]
        i = IDS[key]
        return pltpu.make_async_remote_copy(
            src_ref=src,
            dst_ref=dst,
            send_sem=send.at[i],
            recv_sem=recv.at[i],
            device_id={"tp": peer(h, second, d)},
            device_id_type=pl.DeviceIdType.MESH,
        )

    both = [(h, d) for h in (0, 1) for d in (0, 1)]

    barrier = pltpu.get_barrier_semaphore()
    for h in (0, 1):
        pl.semaphore_signal(
            barrier, inc=1, device_id={"tp": peer(h, False, 1)},
            device_id_type=pl.DeviceIdType.MESH,
        )
    pl.semaphore_wait(barrier, 2)
    for h in (0, 1):
        pl.semaphore_signal(
            below.at[h], inc=1, device_id={"tp": peer(h, False, 0)},
            device_id_type=pl.DeviceIdType.MESH,
        )

    for n in (0, 1):
        for h in (0, 1):
            message(("a", h, 0, n)).start()
    for h in (0, 1):
        pl.semaphore_wait(below.at[h], 1)
        for n in (0, 1):
            message(("a", h, 1, 1 - n)).start()
    weights = [
        pltpu.make_async_copy(src, dst, wsem.at[i])
        for i, (src, dst) in enumerate(((wg_hbm, wg), (wu_hbm, wu), (wd_hbm, wd)))
    ]
    own = [
        pltpu.make_async_copy(x.at[rows(h), :], xbuf.at[rows(h), :], lsem.at[h]) for h in (0, 1)
    ]
    keep = [
        pltpu.make_async_copy(xbuf.at[rows(h), :], blk(xg, h, 0, 0), lsem.at[h]) for h in (0, 1)
    ]
    for c in own:
        c.start()
    for c in own:
        c.wait()
    for c in keep:
        c.start()
    for c in weights:
        c.start()
    for c in keep:
        c.wait()
    for h, d in both:
        message(("a", h, d, d)).wait_recv()
        message(("af", h, d)).start()
    for h, d in both:
        message(("b", h, 0, d)).start()
    for h, d in both:
        message(("a", h, d, 1 - d)).wait_recv()
    for j in (PLUS, MINUS):
        for h, d in both:
            message(("b", h, j, d)).start()
    for c in weights:
        c.wait()
    for h, d in both:
        message(("af", h, d)).wait_recv()
    for h, d in both:
        message(("b", h, 3, d)).start()

    def send_terms(k):
        for m in (1, 2):
            for h, d in both:
                message(("ra", h, k, d, m)).start()

    def arrivals(u):
        for j in range(4):
            @pl.when(u == 1 + j)
            def _():
                for h, d in both:
                    message(("b", h, j, d)).wait_recv()
                    message(("bf", h, j, d)).start()
                if j == 3:
                    send_terms(0)

        for part in (0, 1):
            @pl.when(u == 5 + part)
            def _():
                if part == 1:
                    send_terms(PLUS)
                    send_terms(MINUS)
                for j in (2 * part, 2 * part + 1):
                    for h, d in both:
                        message(("bf", h, j, d)).wait_recv()

    n_up, n_down = 256, stg.shape[2]
    n = depth // n_down

    def stage(u, t, slot):
        c = pl.ds(pl.multiple_of(t * n_down, n_down), n_down)
        return (
            pltpu.make_async_copy(stg.at[slot], tf.at[u, :, c], osem.at[slot]),
            pltpu.make_async_copy(half_stg.at[slot], tb.at[u, :, c], ssem.at[slot]),
        )

    def drain(u):
        for t in (n - 2, n - 1):
            for c in stage(u, t, t % 2):
                c.wait()

    def load(u):
        return pltpu.make_async_copy(xg.at[u], xbuf, xsem)

    load(0).start()

    def unit(u, carry):
        load(u).wait()

        def up_tile(t, carry):
            c = pl.ds(pl.multiple_of(t * n_up, n_up), n_up)
            gate = jnp.dot(xbuf[...], wg[:, c], preferred_element_type=jnp.float32)
            up = jnp.dot(xbuf[...], wu[:, c], preferred_element_type=jnp.float32)
            hid[:, c] = (jax.nn.silu(gate) * up).astype(jnp.bfloat16)
            return carry

        lax.fori_loop(0, ff // n_up, up_tile, 0)

        @pl.when(u > 0)
        def _():
            drain(u - 1)

        arrivals(u)

        @pl.when(u < UNITS - 1)
        def _():
            load(u + 1).start()

        def down_tile(t, carry):
            slot = t % 2

            @pl.when(t >= 2)
            def _():
                for c in stage(u, t - 2, slot):
                    c.wait()

            c = pl.ds(pl.multiple_of(t * n_down, n_down), n_down)
            term = jnp.dot(hid[...], wd[:, c], preferred_element_type=jnp.float32)
            stg[slot] = term
            half_stg[slot] = term.astype(jnp.bfloat16)
            for c in stage(u, t, slot):
                c.start()
            return carry

        lax.fori_loop(0, n, down_tile, 0)
        return carry

    lax.fori_loop(0, UNITS, unit, 0)
    drain(UNITS - 1)

    quarter = fa.shape[2]

    def combine(items, wide_columns=piece):
        step = min(quarter, wide_columns)

        def room(i):
            return rows(i // 4), pl.ds((i % 4) * quarter, step)

        parts = []
        for wide, narrow, to_wide, to_narrow, then in items:
            for q in range(wide_columns // step):
                c = pl.ds(q * step, step)
                cut = lambda ref: None if ref is None else ref.at[:, c]
                parts.append((
                    cut(wide), [cut(r) for r in narrow], cut(to_wide), cut(to_narrow),
                    then if q == wide_columns // step - 1 else None,
                ))

        def loads(i):
            wide, narrow = parts[i][:2]
            s = i % 2
            out = [pltpu.make_async_copy(wide, fa.at[s, :, pl.ds(0, step)], lsem.at[3 * s])]
            for n, ref in enumerate(narrow):
                out.append(pltpu.make_async_copy(
                    ref, xbuf.at[room(3 * s + n)], lsem.at[3 * s + 1 + n]))
            return out

        def stores(i):
            wide, narrow = parts[i][2:4]
            s = i % 2
            out = []
            if wide is not None:
                out.append(pltpu.make_async_copy(fa.at[s, :, pl.ds(0, step)], wide, osem.at[s]))
            if narrow is not None:
                out.append(pltpu.make_async_copy(xbuf.at[room(3 * s + 2)], narrow, ssem.at[s]))
            return out

        def finish(i):
            for c in stores(i):
                c.wait()
            if parts[i][4] is not None:
                parts[i][4].start()

        for c in loads(0):
            c.start()
        for i in range(len(parts)):
            s = i % 2
            if i >= 1:
                finish(i - 1)
            if i + 1 < len(parts):
                for c in loads(i + 1):
                    c.start()
            for c in loads(i):
                c.wait()
            total = fa[s, :, :step]
            for n in range(len(parts[i][1])):
                total = total + xbuf[room(3 * s + n)].astype(jnp.float32)
            if parts[i][2] is not None:
                fa[s, :, :step] = total
            if parts[i][3] is not None:
                xbuf[room(3 * s + 2)] = total.astype(jnp.bfloat16)
            for c in stores(i):
                c.start()
        finish(len(parts) - 1)

    def pass_on(k):
        for h, d in both:
            message(("ra", h, k, d, 1)).wait_recv()
        combine([
            (
                blk(tf, h, k, PLUS if d == 0 else MINUS, d), [a1.at[h, k, d]],
                None, m3.at[h, k, d], message(("ra", h, k, d, 3)),
            )
            for h, d in both
        ])

    def first_sum(k, wide, narrow, then=lambda h, c: None):
        for h, d in both:
            for m in (2, 3):
                message(("ra", h, k, d, m)).wait_recv()
        combine([
            (
                blk(tf, h, k, 0, c),
                [bx.at[h, k, 0, :, col(c)], bx.at[h, k, 1, :, col(c)]],
                rf.at[h, k, :, col(c)] if c in wide else None,
                rb.at[h, k, :, col(c)] if c in narrow else None,
                then(h, c),
            )
            for h in (0, 1) for c in (0, 1)
        ])

    send_terms(3)
    pass_on(0)
    pass_on(PLUS)
    pass_on(3)
    pass_on(MINUS)
    first_sum(0, (0, 1), ())
    first_sum(PLUS, (0,), (1,))
    first_sum(3, (), (0, 1), lambda h, c: message(("rb", h, c, 1)))
    for h in (0, 1):
        message(("rb", h, 0, 2)).start()
    first_sum(MINUS, (1,), (0,), lambda h, c: message(("rb", h, 1, 2)) if c == 0 else None)
    for h, d in both:
        message(("rb", h, d, 1)).wait_recv()
    combine([
        (
            rf.at[h, PLUS if d == 0 else MINUS, :, col(d)], [a1b.at[h, d]],
            None, m3b.at[h, d], message(("rb", h, d, 3)),
        )
        for h, d in both
    ])
    for h, d in both:
        message(("rb", h, d, 4)).start()

    for h, d in both:
        message(("rb", h, d, 2)).wait_recv()
    width = n_down
    spots = [(h, c, q) for h in (0, 1) for c in (0, 1) for q in range(soon // width)]

    def spot(i):
        h, c, q = spots[i]
        return q, rows(2 * h + c)

    def lane(i):
        h, c, q = spots[i]
        return rows(2 * h + c), pl.ds(q * width, width)

    def fetch(i):
        h, c, q = spots[i]
        return (
            pltpu.make_async_copy(
                rf.at[h, 0, :, pl.ds(c * piece + q * width, width)], stg.at[spot(i)], zsem.at[i]),
            pltpu.make_async_copy(
                mid.at[h, 1 - c, :, pl.ds(q * width, width)], xbuf.at[lane(i)],
                zsem.at[len(spots) + i]),
        )

    for i in range(len(spots)):
        for c in fetch(i):
            c.start()
    for i in range(len(spots)):
        for c in fetch(i):
            c.wait()
        stg[spot(i)] = stg[spot(i)] + xbuf[lane(i)].astype(jnp.float32)
    combine([
        (
            rf.at[h, 0, :, pl.ds(c * piece + soon, LATE)],
            [mid.at[h, 1 - c, :, pl.ds(soon, LATE)]],
            most.at[rows(h), pl.ds(c * LATE, LATE)], None, None,
        )
        for h in (0, 1) for c in (0, 1)
    ], LATE)
    for h, d in both:
        message(("rb", h, d, 3)).wait_recv()

    def arrived(i):
        h, c, q = spots[i]
        return pltpu.make_async_copy(
            near.at[h, c, :, pl.ds(q * width, width)], xbuf.at[lane(i)], zsem.at[i])

    def settled(i):
        h, c, q = spots[i]
        return pltpu.make_async_copy(
            xbuf.at[lane(i)], early.at[rows(h), pl.ds(c * soon + q * width, width)],
            zsem.at[len(spots) + i])

    for i in range(len(spots)):
        arrived(i).start()
    for i in range(len(spots)):
        arrived(i).wait()
        total = stg[spot(i)] + xbuf[lane(i)].astype(jnp.float32)
        xbuf[lane(i)] = total.astype(jnp.bfloat16)
        settled(i).start()
    for i in range(len(spots)):
        settled(i).wait()
    last = [("rb", h, d, 4) for h, d in both]
    for key in IDS:
        if key not in last:
            message(key).wait_send()
    for key in last:
        message(key).wait_recv()
    for key in last:
        message(key).wait_send()


def finish(early, most, late, y, rest, add, out, sem):
    rows, columns = most.shape
    piece, soon, cut = y.shape[1] // 2, early.shape[1] // 2, rows // 2
    spots = [(i, c) for i in (0, 1) for c in (0, 1)]

    def part(i, c, n):
        r = pl.ds(i * cut, cut)
        place = (r, pl.ds(c * piece, soon))
        lane = (r, pl.ds(c * LATE, LATE))
        to = (r, pl.ds(c * piece + soon, LATE))
        src, dst = (
            (most.at[lane], rest.at[lane]),
            (late.at[lane], add.at[lane]),
            (early.at[r, pl.ds(c * soon, soon)], out.at[place]),
            (out.at[place], y.at[place]),
            (out.at[to], y.at[to]),
        )[n]
        return pltpu.make_async_copy(src, dst, sem.at[5 * (2 * i + c) + n])

    for i, c in spots:
        for n in (0, 1, 2):
            part(i, c, n).start()
    for i, c in spots:
        part(i, c, 0).wait()
        part(i, c, 1).wait()
        r, lane = pl.ds(i * cut, cut), pl.ds(c * LATE, LATE)
        total = rest[r, lane] + add[r, lane].astype(jnp.float32)
        out[r, pl.ds(c * piece + soon, LATE)] = total.astype(out.dtype)
        part(i, c, 4).start()
        part(i, c, 2).wait()
        part(i, c, 3).start()
    for i, c in spots:
        part(i, c, 3).wait()
        part(i, c, 4).wait()


def solution(mesh):
    side = math.isqrt(mesh.shape["tp"])

    def step(x, w_gate, w_up, w_down):
        rows, depth = x.shape
        ff = w_gate.shape[1]
        half, piece = rows // 2, depth // 2
        bf, f32 = jnp.bfloat16, jnp.float32
        n = len(IDS)
        flops = 6 * rows * side * side * depth * ff
        shapes = [
            ((rows, depth - 2 * LATE), bf),
            ((rows, 2 * LATE), f32),
            ((rows, 2 * LATE), bf),
            ((UNITS, 4 * half, depth), bf),
            ((UNITS, 4 * half, depth), f32),
            ((UNITS, 4 * half, depth), bf),
            ((2, 4, 2, half, piece), bf),
            ((2, 4, 2, half, depth), bf),
            ((2, 4, 2, half, piece), bf),
            ((2, 4, half, depth), f32),
            ((2, 4, half, depth), bf),
            ((2, 2, half, piece), bf),
            ((2, 2, half, piece), bf),
            ((2, 2, half, piece), bf),
            ((2, 2, half, piece - LATE), bf),
        ]
        out = pl.pallas_call(
            functools.partial(kernel, side),
            out_shape=[jax.ShapeDtypeStruct(s, t) for s, t in shapes],
            in_specs=[pl.BlockSpec(memory_space=pl.ANY)] * 4,
            out_specs=[pl.BlockSpec(memory_space=pl.ANY)] * len(shapes),
            scratch_shapes=[
                pltpu.VMEM((depth, ff), bf),
                pltpu.VMEM((depth, ff), bf),
                pltpu.VMEM((ff, depth), bf),
                pltpu.VMEM((4 * half, depth), bf),
                pltpu.VMEM((4 * half, ff), bf),
                pltpu.VMEM((2, 4 * half, depth // 7), f32),
                pltpu.VMEM((2, 4 * half, depth // 7), bf),
                pltpu.VMEM((2, half, piece // 2), f32),
                pltpu.SemaphoreType.DMA((3,)),
                pltpu.SemaphoreType.DMA,
                pltpu.SemaphoreType.DMA((2,)),
                pltpu.SemaphoreType.DMA((2,)),
                pltpu.SemaphoreType.DMA((6,)),
                pltpu.SemaphoreType.DMA((16,)),
                pltpu.SemaphoreType.REGULAR((2,)),
                pltpu.SemaphoreType.DMA((n,)),
                pltpu.SemaphoreType.DMA((n,)),
            ],
            compiler_params=pltpu.CompilerParams(
                collective_id=0, has_side_effects=True, vmem_limit_bytes=VMEM_LIMIT
            ),
            cost_estimate=pl.CostEstimate(
                flops=flops, bytes_accessed=3 * depth * ff * 2, transcendentals=0
            ),
            name="block",
        )(x, w_gate, w_up, w_down)
        return pl.pallas_call(
            finish,
            out_shape=jax.ShapeDtypeStruct((rows, depth), bf),
            in_specs=[pl.BlockSpec(memory_space=pl.ANY)] * 3,
            out_specs=pl.BlockSpec(memory_space=pl.ANY),
            scratch_shapes=[
                pltpu.VMEM((rows, 2 * LATE), f32),
                pltpu.VMEM((rows, 2 * LATE), bf),
                pltpu.VMEM((rows, depth), bf),
                pltpu.SemaphoreType.DMA((20,)),
            ],
            compiler_params=pltpu.CompilerParams(vmem_limit_bytes=VMEM_LIMIT),
            name="finish",
        )(*out[:3])

    return jax.shard_map(
        step,
        mesh=mesh,
        in_specs=(P(("dp", "tp"), None), P(None, "tp"), P(None, "tp"), P("tp", None)),
        out_specs=P(("dp", "tp"), None),
        check_vma=False,
    )
```

```python
import functools
import math

import jax
import jax.numpy as jnp
from jax import lax
from jax.experimental import pallas as pl
from jax.experimental.pallas import tpu as pltpu
from jax.sharding import PartitionSpec as P

OFF = (0, 1, -1, 2)
PLUS, MINUS = 1, 2
LATE = 1536
CUTS = 5
UNITS = 8
VMEM_LIMIT = 67043328


def place(h, k, j):
    if k == 0:
        return h, j
    if k < 3:
        return 2 + j, 2 * h + k - 1
    return 6 + j // 2, 2 * h + j % 2


class Sems:
    def __init__(self):
        self.ids = {}

    def __call__(self, key):
        return self.ids.setdefault(key, len(self.ids))


def message_ids():
    ids = Sems()
    for h in (0, 1):
        for d in (0, 1):
            ids(("af", h, d))
            for c in (0, 1):
                ids(("a", h, d, c))
            for j in range(4):
                ids(("b", h, j, d)), ids(("bf", h, j, d))
            for k in range(4):
                for m in (1, 2, 3):
                    ids(("ra", h, k, d, m))
            for m in (1, 2, 3, 4):
                ids(("rb", h, d, m))
    return ids.ids


IDS = message_ids()


def kernel(
    side, x, wg_hbm, wu_hbm, wd_hbm,
    early, most, late, xg, tf, tb, a1, bx, m3, rf, rb, a1b, m3b, mid, near,
    wg, wu, wd, xbuf, hid, stg, half_stg, fa, wsem, xsem, osem, ssem, lsem, zsem, below, send, recv,
):
    half, depth = x.shape[0] // 2, x.shape[1]
    piece = depth // 2
    soon = piece - LATE
    ff = wg_hbm.shape[1]
    me = lax.axis_index("tp")
    mx, my = me // side, me % side

    def peer(h, second, d):
        step = 1 if d == 0 else side - 1
        if (h == 0) != second:
            return ((mx + step) % side) * side + my
        return mx * side + (my + step) % side

    def col(c):
        return pl.ds(c * piece, piece)

    def rows(s):
        return pl.ds(s * half, half)

    def blk(buf, h, k, j, c=None):
        u, s = place(h, k, j)
        if c is None:
            return buf.at[u, rows(s), :]
        return buf.at[u, rows(s), col(c)]

    def message(key):
        kind, h, d = key[0], key[1], key[3] if key[0] in ("b", "bf", "ra") else key[2]
        second = kind in ("b", "bf", "rb")
        here = PLUS if d == 0 else MINUS
        back = MINUS if d == 0 else PLUS
        if kind == "a":
            c = key[3]
            src, dst = x.at[rows(h), col(c)], blk(xg, h, 0, back, c)
        elif kind == "af":
            src, dst = blk(xg, h, 0, back, d), blk(xg, h, 0, 3, d)
        elif kind == "b":
            j = key[2]
            src = x.at[rows(h), :] if j == 0 else blk(xg, h, 0, j)
            dst = blk(xg, h, back, j)
        elif kind == "bf":
            j = key[2]
            src, dst = blk(xg, h, back, j, d), blk(xg, h, 3, j, d)
        elif kind == "ra":
            k, m = key[2], key[4]
            if m == 1:
                src, dst = blk(tb, h, k, 3, d), a1.at[h, k, d]
            elif m == 2:
                src, dst = blk(tb, h, k, here, 1 - d), bx.at[h, k, d, :, col(1 - d)]
            else:
                src, dst = m3.at[h, k, d], bx.at[h, k, d, :, col(d)]
        else:
            m = key[3]
            if m == 1:
                src, dst = rb.at[h, 3, :, col(d)], a1b.at[h, d]
            elif m == 2:
                src, dst = rb.at[h, here, :, col(1 - d)], mid.at[h, d]
            elif m == 3:
                src, dst = m3b.at[h, d, :, pl.ds(0, soon)], near.at[h, d]
            else:
                src = m3b.at[h, d, :, pl.ds(soon, LATE)]
                dst = late.at[rows(h), pl.ds(d * LATE, LATE)]
        i = IDS[key]
        return pltpu.make_async_remote_copy(
            src_ref=src,
            dst_ref=dst,
            send_sem=send.at[i],
            recv_sem=recv.at[i],
            device_id={"tp": peer(h, second, d)},
            device_id_type=pl.DeviceIdType.MESH,
        )

    both = [(h, d) for h in (0, 1) for d in (0, 1)]

    barrier = pltpu.get_barrier_semaphore()
    for h in (0, 1):
        pl.semaphore_signal(
            barrier, inc=1, device_id={"tp": peer(h, False, 1)},
            device_id_type=pl.DeviceIdType.MESH,
        )
    pl.semaphore_wait(barrier, 2)
    for h in (0, 1):
        pl.semaphore_signal(
            below.at[h], inc=1, device_id={"tp": peer(h, False, 0)},
            device_id_type=pl.DeviceIdType.MESH,
        )

    for n in (0, 1):
        for h in (0, 1):
            message(("a", h, 0, n)).start()
    for h in (0, 1):
        pl.semaphore_wait(below.at[h], 1)
        for n in (0, 1):
            message(("a", h, 1, 1 - n)).start()
    weights = [
        pltpu.make_async_copy(src, dst, wsem.at[i])
        for i, (src, dst) in enumerate(((wg_hbm, wg), (wu_hbm, wu), (wd_hbm, wd)))
    ]
    own = [
        pltpu.make_async_copy(x.at[rows(h), :], xbuf.at[rows(h), :], lsem.at[h]) for h in (0, 1)
    ]
    keep = [
        pltpu.make_async_copy(xbuf.at[rows(h), :], blk(xg, h, 0, 0), lsem.at[h]) for h in (0, 1)
    ]
    for c in own:
        c.start()
    for c in own:
        c.wait()
    for c in keep:
        c.start()
    for c in weights:
        c.start()
    for c in keep:
        c.wait()
    for h, d in both:
        message(("a", h, d, d)).wait_recv()
        message(("af", h, d)).start()
    for h, d in both:
        message(("b", h, 0, d)).start()
    for h, d in both:
        message(("a", h, d, 1 - d)).wait_recv()
    for j in (PLUS, MINUS):
        for h, d in both:
            message(("b", h, j, d)).start()
    for c in weights:
        c.wait()
    for h, d in both:
        message(("af", h, d)).wait_recv()
    for h, d in both:
        message(("b", h, 3, d)).start()

    def send_terms(k):
        for m in (1, 2):
            for h, d in both:
                message(("ra", h, k, d, m)).start()

    def arrivals(u):
        for j in range(4):
            @pl.when(u == 1 + j)
            def _():
                for h, d in both:
                    message(("b", h, j, d)).wait_recv()
                    message(("bf", h, j, d)).start()
                if j == 3:
                    send_terms(0)

        for part in (0, 1):
            @pl.when(u == 5 + part)
            def _():
                if part == 1:
                    send_terms(PLUS)
                    send_terms(MINUS)
                for j in (2 * part, 2 * part + 1):
                    for h, d in both:
                        message(("bf", h, j, d)).wait_recv()

    n_up, n_down = 256, stg.shape[2]
    n = depth // n_down

    def stage(u, t, slot):
        c = pl.ds(pl.multiple_of(t * n_down, n_down), n_down)
        return (
            pltpu.make_async_copy(stg.at[slot], tf.at[u, :, c], osem.at[slot]),
            pltpu.make_async_copy(half_stg.at[slot], tb.at[u, :, c], ssem.at[slot]),
        )

    def drain(u):
        for t in (n - 2, n - 1):
            for c in stage(u, t, t % 2):
                c.wait()

    def load(u):
        return pltpu.make_async_copy(xg.at[u], xbuf, xsem)

    load(0).start()

    def unit(u, carry):
        load(u).wait()

        def up_tile(t, carry):
            c = pl.ds(pl.multiple_of(t * n_up, n_up), n_up)
            gate = jnp.dot(xbuf[...], wg[:, c], preferred_element_type=jnp.float32)
            up = jnp.dot(xbuf[...], wu[:, c], preferred_element_type=jnp.float32)
            hid[:, c] = (jax.nn.silu(gate) * up).astype(jnp.bfloat16)
            return carry

        lax.fori_loop(0, ff // n_up, up_tile, 0)

        @pl.when(u > 0)
        def _():
            drain(u - 1)

        arrivals(u)

        @pl.when(u < UNITS - 1)
        def _():
            load(u + 1).start()

        def down_tile(t, carry):
            slot = t % 2

            @pl.when(t >= 2)
            def _():
                for c in stage(u, t - 2, slot):
                    c.wait()

            c = pl.ds(pl.multiple_of(t * n_down, n_down), n_down)
            term = jnp.dot(hid[...], wd[:, c], preferred_element_type=jnp.float32)
            stg[slot] = term
            half_stg[slot] = term.astype(jnp.bfloat16)
            for c in stage(u, t, slot):
                c.start()
            return carry

        lax.fori_loop(0, n, down_tile, 0)
        return carry

    lax.fori_loop(0, UNITS, unit, 0)
    drain(UNITS - 1)

    quarter = fa.shape[2]

    def combine(items, wide_columns=piece):
        step = min(quarter, wide_columns)

        def room(i):
            return rows(i // 4), pl.ds((i % 4) * quarter, step)

        parts = []
        for wide, narrow, to_wide, to_narrow, then in items:
            for q in range(wide_columns // step):
                c = pl.ds(q * step, step)
                cut = lambda ref: None if ref is None else ref.at[:, c]
                parts.append((
                    cut(wide), [cut(r) for r in narrow], cut(to_wide), cut(to_narrow),
                    then if q == wide_columns // step - 1 else None,
                ))

        def loads(i):
            wide, narrow = parts[i][:2]
            s = i % 2
            out = [pltpu.make_async_copy(wide, fa.at[s, :, pl.ds(0, step)], lsem.at[3 * s])]
            for n, ref in enumerate(narrow):
                out.append(pltpu.make_async_copy(
                    ref, xbuf.at[room(3 * s + n)], lsem.at[3 * s + 1 + n]))
            return out

        def stores(i):
            wide, narrow = parts[i][2:4]
            s = i % 2
            out = []
            if wide is not None:
                out.append(pltpu.make_async_copy(fa.at[s, :, pl.ds(0, step)], wide, osem.at[s]))
            if narrow is not None:
                out.append(pltpu.make_async_copy(xbuf.at[room(3 * s + 2)], narrow, ssem.at[s]))
            return out

        def finish(i):
            for c in stores(i):
                c.wait()
            if parts[i][4] is not None:
                parts[i][4].start()

        for c in loads(0):
            c.start()
        for i in range(len(parts)):
            s = i % 2
            if i >= 1:
                finish(i - 1)
            if i + 1 < len(parts):
                for c in loads(i + 1):
                    c.start()
            for c in loads(i):
                c.wait()
            total = fa[s, :, :step]
            for n in range(len(parts[i][1])):
                total = total + xbuf[room(3 * s + n)].astype(jnp.float32)
            if parts[i][2] is not None:
                fa[s, :, :step] = total
            if parts[i][3] is not None:
                xbuf[room(3 * s + 2)] = total.astype(jnp.bfloat16)
            for c in stores(i):
                c.start()
        finish(len(parts) - 1)

    def pass_on(k):
        for h, d in both:
            message(("ra", h, k, d, 1)).wait_recv()
        combine([
            (
                blk(tf, h, k, PLUS if d == 0 else MINUS, d), [a1.at[h, k, d]],
                None, m3.at[h, k, d], message(("ra", h, k, d, 3)),
            )
            for h, d in both
        ])

    def first_sum(k, wide, narrow, then=lambda h, c: None):
        for h, d in both:
            for m in (2, 3):
                message(("ra", h, k, d, m)).wait_recv()
        combine([
            (
                blk(tf, h, k, 0, c),
                [bx.at[h, k, 0, :, col(c)], bx.at[h, k, 1, :, col(c)]],
                rf.at[h, k, :, col(c)] if c in wide else None,
                rb.at[h, k, :, col(c)] if c in narrow else None,
                then(h, c),
            )
            for h in (0, 1) for c in (0, 1)
        ])

    send_terms(3)
    pass_on(0)
    pass_on(PLUS)
    pass_on(3)
    pass_on(MINUS)
    first_sum(0, (0, 1), ())
    first_sum(PLUS, (0,), (1,))
    first_sum(3, (), (0, 1), lambda h, c: message(("rb", h, c, 1)))
    for h in (0, 1):
        message(("rb", h, 0, 2)).start()
    first_sum(MINUS, (1,), (0,), lambda h, c: message(("rb", h, 1, 2)) if c == 0 else None)
    for h, d in both:
        message(("rb", h, d, 1)).wait_recv()
    combine([
        (
            rf.at[h, PLUS if d == 0 else MINUS, :, col(d)], [a1b.at[h, d]],
            None, m3b.at[h, d], message(("rb", h, d, 3)),
        )
        for h, d in both
    ])
    for h, d in both:
        message(("rb", h, d, 4)).start()

    for h, d in both:
        message(("rb", h, d, 2)).wait_recv()
    width = n_down
    spots = [(h, c, q) for h in (0, 1) for c in (0, 1) for q in range(soon // width)]

    def spot(i):
        h, c, q = spots[i]
        return q, rows(2 * h + c)

    def lane(i):
        h, c, q = spots[i]
        return rows(2 * h + c), pl.ds(q * width, width)

    def fetch(i):
        h, c, q = spots[i]
        return (
            pltpu.make_async_copy(
                rf.at[h, 0, :, pl.ds(c * piece + q * width, width)], stg.at[spot(i)], zsem.at[i]),
            pltpu.make_async_copy(
                mid.at[h, 1 - c, :, pl.ds(q * width, width)], xbuf.at[lane(i)],
                zsem.at[len(spots) + i]),
        )

    for i in range(len(spots)):
        for c in fetch(i):
            c.start()
    for i in range(len(spots)):
        for c in fetch(i):
            c.wait()
        stg[spot(i)] = stg[spot(i)] + xbuf[lane(i)].astype(jnp.float32)
    combine([
        (
            rf.at[h, 0, :, pl.ds(c * piece + soon, LATE)],
            [mid.at[h, 1 - c, :, pl.ds(soon, LATE)]],
            most.at[rows(h), pl.ds(c * LATE, LATE)], None, None,
        )
        for h in (0, 1) for c in (0, 1)
    ], LATE)
    for h, d in both:
        message(("rb", h, d, 3)).wait_recv()

    def arrived(i):
        h, c, q = spots[i]
        return pltpu.make_async_copy(
            near.at[h, c, :, pl.ds(q * width, width)], xbuf.at[lane(i)], zsem.at[i])

    def settled(i):
        h, c, q = spots[i]
        return pltpu.make_async_copy(
            xbuf.at[lane(i)], early.at[rows(h), pl.ds(c * soon + q * width, width)],
            zsem.at[len(spots) + i])

    for i in range(len(spots)):
        arrived(i).start()
    for i in range(len(spots)):
        arrived(i).wait()
        total = stg[spot(i)] + xbuf[lane(i)].astype(jnp.float32)
        xbuf[lane(i)] = total.astype(jnp.bfloat16)
        settled(i).start()
    for i in range(len(spots)):
        settled(i).wait()
    last = [("rb", h, d, 4) for h, d in both]
    for key in IDS:
        if key not in last:
            message(key).wait_send()
    for key in last:
        message(key).wait_recv()
    for key in last:
        message(key).wait_send()


def finish(early, most, late, y, rest, add, out, sem):
    rows, columns = most.shape
    piece, soon, cut = y.shape[1] // 2, early.shape[1] // 2, rows // CUTS
    spots = [(i, c) for i in range(CUTS) for c in (0, 1)]

    def part(i, c, n):
        r = pl.ds(i * cut, cut)
        place = (r, pl.ds(c * piece, soon))
        lane = (r, pl.ds(c * LATE, LATE))
        to = (r, pl.ds(c * piece + soon, LATE))
        src, dst = (
            (most.at[lane], rest.at[lane]),
            (late.at[lane], add.at[lane]),
            (early.at[r, pl.ds(c * soon, soon)], out.at[place]),
            (out.at[place], y.at[place]),
            (out.at[to], y.at[to]),
        )[n]
        return pltpu.make_async_copy(src, dst, sem.at[5 * (2 * i + c) + n])

    for i, c in spots:
        part(i, c, 2).start()
    for i, c in spots:
        for n in (0, 1):
            part(i, c, n).start()
    for i, c in spots:
        part(i, c, 2).wait()
        part(i, c, 3).start()
    for i, c in spots:
        part(i, c, 0).wait()
        part(i, c, 1).wait()
        r, lane = pl.ds(i * cut, cut), pl.ds(c * LATE, LATE)
        total = rest[r, lane] + add[r, lane].astype(jnp.float32)
        out[r, pl.ds(c * piece + soon, LATE)] = total.astype(out.dtype)
        part(i, c, 4).start()
    for i, c in spots:
        part(i, c, 3).wait()
        part(i, c, 4).wait()


def solution(mesh):
    side = math.isqrt(mesh.shape["tp"])

    def step(x, w_gate, w_up, w_down):
        rows, depth = x.shape
        ff = w_gate.shape[1]
        half, piece = rows // 2, depth // 2
        bf, f32 = jnp.bfloat16, jnp.float32
        n = len(IDS)
        flops = 6 * rows * side * side * depth * ff
        shapes = [
            ((rows, depth - 2 * LATE), bf),
            ((rows, 2 * LATE), f32),
            ((rows, 2 * LATE), bf),
            ((UNITS, 4 * half, depth), bf),
            ((UNITS, 4 * half, depth), f32),
            ((UNITS, 4 * half, depth), bf),
            ((2, 4, 2, half, piece), bf),
            ((2, 4, 2, half, depth), bf),
            ((2, 4, 2, half, piece), bf),
            ((2, 4, half, depth), f32),
            ((2, 4, half, depth), bf),
            ((2, 2, half, piece), bf),
            ((2, 2, half, piece), bf),
            ((2, 2, half, piece), bf),
            ((2, 2, half, piece - LATE), bf),
        ]
        out = pl.pallas_call(
            functools.partial(kernel, side),
            out_shape=[jax.ShapeDtypeStruct(s, t) for s, t in shapes],
            in_specs=[pl.BlockSpec(memory_space=pl.ANY)] * 4,
            out_specs=[pl.BlockSpec(memory_space=pl.ANY)] * len(shapes),
            scratch_shapes=[
                pltpu.VMEM((depth, ff), bf),
                pltpu.VMEM((depth, ff), bf),
                pltpu.VMEM((ff, depth), bf),
                pltpu.VMEM((4 * half, depth), bf),
                pltpu.VMEM((4 * half, ff), bf),
                pltpu.VMEM((2, 4 * half, depth // 7), f32),
                pltpu.VMEM((2, 4 * half, depth // 7), bf),
                pltpu.VMEM((2, half, piece // 2), f32),
                pltpu.SemaphoreType.DMA((3,)),
                pltpu.SemaphoreType.DMA,
                pltpu.SemaphoreType.DMA((2,)),
                pltpu.SemaphoreType.DMA((2,)),
                pltpu.SemaphoreType.DMA((6,)),
                pltpu.SemaphoreType.DMA((16,)),
                pltpu.SemaphoreType.REGULAR((2,)),
                pltpu.SemaphoreType.DMA((n,)),
                pltpu.SemaphoreType.DMA((n,)),
            ],
            compiler_params=pltpu.CompilerParams(
                collective_id=0, has_side_effects=True, vmem_limit_bytes=VMEM_LIMIT
            ),
            cost_estimate=pl.CostEstimate(
                flops=flops, bytes_accessed=3 * depth * ff * 2, transcendentals=0
            ),
            name="block",
        )(x, w_gate, w_up, w_down)
        return pl.pallas_call(
            finish,
            out_shape=jax.ShapeDtypeStruct((rows, depth), bf),
            in_specs=[pl.BlockSpec(memory_space=pl.ANY)] * 3,
            out_specs=pl.BlockSpec(memory_space=pl.ANY),
            scratch_shapes=[
                pltpu.VMEM((rows, 2 * LATE), f32),
                pltpu.VMEM((rows, 2 * LATE), bf),
                pltpu.VMEM((rows, depth), bf),
                pltpu.SemaphoreType.DMA((10 * CUTS,)),
            ],
            compiler_params=pltpu.CompilerParams(vmem_limit_bytes=VMEM_LIMIT),
            name="finish",
        )(*out[:3])

    return jax.shard_map(
        step,
        mesh=mesh,
        in_specs=(P(("dp", "tp"), None), P(None, "tp"), P(None, "tp"), P("tp", None)),
        out_specs=P(("dp", "tp"), None),
        check_vma=False,
    )
```
